32 devices in a mesh: batch: 4 (over y, x), ctx: 8 (over z, core).
Axes of the slice: x: 2, y: 2, z: 4, core: 2. Of those that a mesh axis runs over, the one named last changes fastest.
Arguments:
- asked_for: bfloat16 [4, 1024, 64, 64], P('batch', 'ctx'), may hold values from -6 to 6
- offered: bfloat16 [4, 1024, 64, 64], P('batch', 'ctx'), may hold values from -6 to 6
- contents: bfloat16 [4, 1024, 64, 64], P('batch', 'ctx'), may hold values from -6 to 6
- out_weight: bfloat16 [4096, 4096], P('batch'), may hold values from -0.09375 to 0.09375
Outputs:
- layer_out: bfloat16 [4, 1024, 4096], P('batch', 'ctx')
The draws below stay inside these ranges and needn't reach their ends.
All inputs are finite; a program needn't handle non-finite values.
Results may differ from the reference program's by a relative error of at most 0.006.
Values may be sent and summed in bfloat16 or wider, within the bound.
A program may use at most 128 MiB of HBM per device.

```python
import jax
import jax.numpy as jnp
from jax import lax

HEADS = 64
HEAD_SIZE = 64
BATCH = 4
TOKENS = 1024
WIDTH = 4096


def shard_levels(key, dims, split, least, top_value):
    level = 1.0
    for axis_at, shards_of in split:
        steps = jax.random.uniform(jax.random.fold_in(jax.random.fold_in(key, 6), axis_at), (shards_of,), jnp.float32, least / len(split), top_value / len(split))
        level = level * jnp.repeat(jnp.exp(steps), dims[axis_at] // shards_of).reshape((-1,) + (1,) * (len(dims) - 1 - axis_at))
    return level


def centred(rng, extent, width, bound, pieces=(), kind=jnp.bfloat16):
    entries = jax.random.normal(rng, extent, jnp.float32) * width
    if len(pieces) > 0:
        entries = shard_levels(rng, extent, pieces, -0.22, 0.18) * entries
    return jnp.clip(entries, min=-bound, max=bound).astype(kind)


def setup_inputs(seed: int = 0) -> dict:
    key_of = jax.random.split(jax.random.key(seed), 5)
    return {
        "asked_for": centred(key_of[0], (BATCH, TOKENS, HEADS, HEAD_SIZE), 1.0, 6.0, ((0, 4), (1, 8))),
        "offered": centred(key_of[1], (BATCH, TOKENS, HEADS, HEAD_SIZE), 1.0, 6.0, ((0, 4), (1, 8))),
        "contents": centred(key_of[2], (BATCH, TOKENS, HEADS, HEAD_SIZE), 1.0, 6.0, ((0, 4), (1, 8))),
        "out_weight": centred(key_of[3], (WIDTH, WIDTH), WIDTH ** -0.5, 0.09375, ((0, 4),)),
    }


def to_features(values):
    wide = values.astype(jnp.float32)
    return (jax.nn.softplus(wide)).astype(jnp.bfloat16)


def after_reading(read, count):
    result = read * count ** 0.5
    return result.astype(jnp.bfloat16)


def look_up(features, state, mass):
    small = lax.optimization_barrier(state.astype(jnp.bfloat16))
    top = jnp.einsum("bthd,bhde->bthe", features.astype(jnp.float32), small.astype(jnp.float32))
    bottom = jnp.einsum("bthd,bhd->bth", features.astype(jnp.float32), mass, precision=lax.Precision.HIGHEST)
    return top / (bottom + 1e-3)[..., None]


def reference(asked_for, offered, contents, out_weight):
    query_feature, key_feature = lax.optimization_barrier((to_features(asked_for), to_features(offered)))
    state = jnp.einsum("bthd,bthe->bhde", key_feature.astype(jnp.float32), contents.astype(jnp.float32)) / TOKENS
    mass = jnp.sum(key_feature.astype(jnp.float32), axis=1) / TOKENS
    mixed = after_reading(look_up(query_feature, state, mass), TOKENS).reshape(BATCH, TOKENS, WIDTH)
    mixed = lax.optimization_barrier(mixed)
    layer_out = jnp.einsum("btw,wv->btv", mixed.astype(jnp.float32), out_weight.astype(jnp.float32)).astype(jnp.bfloat16)
    return layer_out
```

```python
import functools

import jax
import jax.numpy as jnp
from jax import lax
from jax.experimental import pallas as pl
from jax.experimental.pallas import tpu as pltpu
from jax.sharding import PartitionSpec as P

MESH = pl.DeviceIdType.MESH
LANES = 128
EXTRA = 16
CHUNK = 512


def softplus(x):
    x = x.astype(jnp.float32)
    return (jnp.maximum(x, 0.0) + jnp.log(1.0 + jnp.exp(-jnp.abs(x)))).astype(jnp.bfloat16)


def split_mass(m):
    row = lax.broadcasted_iota(jnp.int32, (EXTRA, LANES), 0)
    high = m.astype(jnp.bfloat16).astype(jnp.float32)
    return jnp.where(row == 0, high, jnp.where(row == 1, m - high, 0.0)).astype(jnp.bfloat16)


def kernel(
    nb, nc, size, q_ref, k_ref, v_ref, w_ref, o_ref,
    kt, vt, wv, qx, part, rs, own, st, mixed, out_buf, mine, in_buf,
    local_sem, q_send, q_recv, rs_send, rs_recv, ag_send, ag_recv, pr_send, pr_recv,
):
    b, c = lax.axis_index("batch"), lax.axis_index("ctx")
    rows, tokens = k_ref.shape
    pairs = rows // LANES
    ppg, ppd = pairs // nb, pairs // nc
    group = rows // nb
    total = nb * nc
    me = b * nc + c
    count = tokens * nc
    chunks = out_buf.shape[0]

    barrier = pltpu.get_barrier_semaphore()

    def greet(i, carry):
        d = lax.rem(me + i, total)
        pl.semaphore_signal(barrier, inc=1, device_id=(d // nc, lax.rem(d, nc)), device_id_type=MESH)
        return carry

    lax.fori_loop(1, total, greet, 0)
    k_copy = pltpu.make_async_copy(k_ref, kt, local_sem.at[0])
    v_copy = pltpu.make_async_copy(v_ref, vt, local_sem.at[1])
    q_copy = pltpu.make_async_copy(q_ref.at[pl.ds(b * group, group)], qx.at[0], local_sem.at[2])
    w_copy = pltpu.make_async_copy(w_ref, wv, local_sem.at[3])
    k_copy.start()
    v_copy.start()
    q_copy.start()
    w_copy.start()
    pl.semaphore_wait(barrier, total - 1)

    def q_move(k):
        to = lax.rem(b + k, nb)
        return pltpu.make_async_remote_copy(
            src_ref=q_ref.at[pl.ds(to * group, group)], dst_ref=qx.at[nb - k],
            send_sem=q_send.at[k], recv_sem=q_recv.at[nb - k],
            device_id=(to, c), device_id_type=MESH,
        )

    for k in range(1, nb):
        q_move(k).start()

    lane = lax.broadcasted_iota(jnp.int32, (size, LANES), 1) < size
    lane_x = lax.broadcasted_iota(jnp.int32, (EXTRA, LANES), 1) < size
    row_x = lax.broadcasted_iota(jnp.int32, (EXTRA, LANES), 0)
    ones = jnp.ones((EXTRA, tokens), jnp.bfloat16)

    def rs_move(k):
        to = lax.rem(c + k, nc)
        return pltpu.make_async_remote_copy(
            src_ref=part.at[to], dst_ref=rs.at[k],
            send_sem=rs_send.at[k], recv_sem=rs_recv.at[k],
            device_id=(b, to), device_id_type=MESH,
        )

    k_copy.wait()
    v_copy.wait()

    def partials(k, carry):
        to = lax.rem(c + k, nc)
        for i in range(ppd):
            at = pl.multiple_of((i * nc + to) * LANES, LANES)
            feature = softplus(kt[pl.ds(at, LANES), :])
            left = jnp.concatenate([vt[pl.ds(at, LANES), :], ones], axis=0)
            s = lax.dot_general(left, feature, (((1,), (1,)), ((), ())), preferred_element_type=jnp.float32)
            part[to, i, :size, :] = jnp.where(lane, s[:size], s[size : 2 * size]).astype(jnp.bfloat16)
            part[to, i, size:, :] = split_mass(s[2 * size :])

        @pl.when(k > 1)
        def _():
            rs_move(k - 1).start()

        return carry

    lax.fori_loop(1, nc + 1, partials, 0)

    for k in range(1, nc):
        rs_move(k).wait_recv()
    for i in range(ppd):
        s = part[c, i].astype(jnp.float32)
        for k in range(1, nc):
            s = s + rs[k, i].astype(jnp.float32)
        s = s / count
        own[i, :size, :] = s[:size].astype(jnp.bfloat16)
        m = jnp.broadcast_to(s[size : size + 1] + s[size + 1 : size + 2], (EXTRA, LANES))
        own[i, size:, :] = split_mass(m)

    def ag_move(i, k):
        p = i * nc + c
        g, slot = p // ppg, lax.rem(p, ppg)
        to = lax.rem(c + k, nc)
        landing = b * ppg + slot
        remote = pltpu.make_async_remote_copy(
            src_ref=own.at[i], dst_ref=st.at[landing],
            send_sem=ag_send.at[i * nc + k], recv_sem=ag_recv.at[landing],
            device_id=(g, to), device_id_type=MESH,
        )
        local = pltpu.make_async_copy(own.at[i], st.at[landing], ag_recv.at[landing])
        return g, remote, local

    for k in range(nc):
        for i in range(ppd):
            g, remote, local = ag_move(i, k)
            if k > 0:
                remote.start()
            else:
                pl.when(g != b)(remote.start)
                pl.when(g == b)(local.start)

    for k in range(nb):
        if k == 0:
            q_copy.wait()
        else:
            q_move(nb - k).wait_recv()

        def featured(i, carry):
            at = pl.multiple_of(i * LANES, LANES)
            qx[k, pl.ds(at, LANES), :] = softplus(qx[k, pl.ds(at, LANES), :])
            return carry

        lax.fori_loop(0, ppg, featured, 0)

    for k in range(nb):
        s = lax.rem(b + k, nb)
        for slot in range(ppg):
            at = s * ppg + slot
            pltpu.make_async_copy(st.at[at], st.at[at], ag_recv.at[at]).wait()
            state = st[at, :size, :]
            mass = st[at, size:, :].astype(jnp.float32)
            hi, lo = mass[0:1], mass[1:2]
            low_half = jnp.where(lane_x, jnp.where(row_x == 0, hi, lo), 0.0)
            high_half = jnp.where(lane_x, 0.0, jnp.where(row_x == 2, hi, lo))
            m = jnp.where(row_x < 2, low_half, jnp.where(row_x < 4, high_half, 0.0)).astype(jnp.bfloat16)
            zero = jnp.zeros_like(state)
            left = jnp.concatenate([jnp.where(lane, state, zero), jnp.where(lane, zero, state), m], axis=0)
            both = lax.dot_general(
                left, qx[k, slot * LANES : (slot + 1) * LANES, :], (((1,), (0,)), ((), ())),
                preferred_element_type=jnp.float32,
            )
            low = both[2 * size :]
            first = count**0.5 / (low[0:1] + low[1:2] + 0.001)
            second = count**0.5 / (low[2:3] + low[3:4] + 0.001)
            read = jnp.concatenate([both[:size] * first, both[size : 2 * size] * second], axis=0)
            mixed[k * tokens : (k + 1) * tokens, slot * LANES : (slot + 1) * LANES] = read.T.astype(jnp.bfloat16)

    def pr_move(j, k):
        return pltpu.make_async_remote_copy(
            src_ref=out_buf.at[j, k - 1], dst_ref=in_buf.at[j, k - 1],
            send_sem=pr_send.at[j, k - 1], recv_sem=pr_recv.at[j, k - 1],
            device_id=(lax.rem(b + k, nb), c), device_id_type=MESH,
        )

    w_copy.wait()
    width = o_ref.shape[1] // chunks

    def project(j, carry):
        at = pl.multiple_of(j * width, width)
        y = jnp.dot(mixed[...], wv[:, pl.ds(at, width)], preferred_element_type=jnp.float32)
        for k in range(1, nb):
            out_buf[j, k - 1] = y[k * tokens : (k + 1) * tokens].astype(jnp.bfloat16)
        mine[:, pl.ds(at, width)] = y[:tokens]
        for k in range(1, nb):
            pr_move(j, k).start()
        return carry

    lax.fori_loop(0, chunks, project, 0)

    def collect(j, carry):
        at = pl.multiple_of(j * width, width)
        y = mine[:, pl.ds(at, width)]
        for k in range(1, nb):
            pr_move(j, k).wait_recv()
            y = y + in_buf[j, k - 1].astype(jnp.float32)
        o_ref[:, pl.ds(at, width)] = y.astype(jnp.bfloat16)
        return carry

    lax.fori_loop(0, chunks, collect, 0)

    for k in range(1, nb):
        q_move(k).wait_send()

    def rs_end(k, carry):
        rs_move(k).wait_send()
        return carry

    lax.fori_loop(1, nc, rs_end, 0)
    for k in range(nc):
        for i in range(ppd):
            g, remote, local = ag_move(i, k)
            if k > 0:
                remote.wait_send()
            else:
                pl.when(g != b)(remote.wait_send)

    def pr_end(j, carry):
        for k in range(1, nb):
            pr_move(j, k).wait_send()
        return carry

    lax.fori_loop(0, chunks, pr_end, 0)


def solution(mesh):
    nb, nc = mesh.shape["batch"], mesh.shape["ctx"]

    def shards(asked_for, offered, contents, out_weight):
        _, tokens, heads, size = asked_for.shape
        rows = heads * size
        depth, columns = out_weight.shape
        pairs = rows // LANES
        block = size + EXTRA
        width = CHUNK if columns % CHUNK == 0 else columns
        chunks = columns // width

        def flat(x):
            return x.transpose(0, 2, 3, 1).reshape(rows, tokens)

        bf16, f32 = jnp.bfloat16, jnp.float32
        dma = pltpu.SemaphoreType.DMA
        out = pl.pallas_call(
            functools.partial(kernel, nb, nc, size),
            out_shape=jax.ShapeDtypeStruct((tokens, columns), bf16),
            in_specs=[pl.BlockSpec(memory_space=pl.ANY)] * 4,
            out_specs=pl.BlockSpec(memory_space=pltpu.VMEM),
            scratch_shapes=[
                pltpu.VMEM((rows, tokens), bf16),
                pltpu.VMEM((rows, tokens), bf16),
                pltpu.VMEM((depth, columns), bf16),
                pltpu.VMEM((nb, rows // nb, tokens), bf16),
                pltpu.VMEM((nc, pairs // nc, block, LANES), bf16),
                pltpu.VMEM((nc, pairs // nc, block, LANES), bf16),
                pltpu.VMEM((pairs // nc, block, LANES), bf16),
                pltpu.VMEM((pairs, block, LANES), bf16),
                pltpu.VMEM((nb * tokens, rows // nb), bf16),
                pltpu.VMEM((chunks, nb - 1, tokens, width), bf16),
                pltpu.VMEM((tokens, columns), f32),
                pltpu.VMEM((chunks, nb - 1, tokens, width), bf16),
                dma((4,)),
                dma((nb,)),
                dma((nb,)),
                dma((nc,)),
                dma((nc,)),
                dma((pairs,)),
                dma((pairs,)),
                dma((chunks, nb - 1)),
                dma((chunks, nb - 1)),
            ],
            compiler_params=pltpu.CompilerParams(
                collective_id=0, has_side_effects=True, vmem_limit_bytes=60 * 2**20
            ),
        )(flat(asked_for), flat(offered), flat(contents), out_weight)
        return out[None]

    in_specs = (
        P("batch", "ctx", None, None),
        P("batch", "ctx", None, None),
        P("batch", "ctx", None, None),
        P("batch", None),
    )
    return jax.shard_map(
        shards, mesh=mesh, in_specs=in_specs, out_specs=P("batch", "ctx", None), check_vma=False
    )
```

```python
import functools
import math

import jax
import jax.numpy as jnp
from jax import lax
from jax.experimental import pallas as pl
from jax.experimental.pallas import tpu as pltpu
from jax.sharding import PartitionSpec as P

MESH = pl.DeviceIdType.MESH
LANES = 128
EXTRA = 16
CHUNK = 512


def softplus(x):
    x = x.astype(jnp.float32)
    return (jnp.maximum(x, 0.0) + jnp.log(1.0 + jnp.exp(-jnp.abs(x)))).astype(jnp.bfloat16)


def split_mass(m):
    row = lax.broadcasted_iota(jnp.int32, (EXTRA, LANES), 0)
    high = m.astype(jnp.bfloat16).astype(jnp.float32)
    return jnp.where(row == 0, high, jnp.where(row == 1, m - high, 0.0)).astype(jnp.bfloat16)


def kernel(
    ny, nx, nc, size, q_ref, k_ref, v_ref, w_ref, o_ref,
    kt, vt, wv, qx, part, rs, own, st, mixed, mine, stage1, stage2,
    local_sem, q_send, q_recv, rs_send, rs_recv, ag_send, ag_recv,
):
    b, c = lax.axis_index("batch"), lax.axis_index("ctx")
    nb = ny * nx
    rows, tokens = k_ref.shape
    pairs = rows // LANES
    ppg, ppd = pairs // nb, pairs // nc
    group = rows // nb
    total = nb * nc
    me = b * nc + c
    count = tokens * nc
    chunks = mine[0].shape[0]

    barrier = pltpu.get_barrier_semaphore()

    def greet(i, carry):
        d = lax.rem(me + i, total)
        pl.semaphore_signal(barrier, inc=1, device_id=(d // nc, lax.rem(d, nc)), device_id_type=MESH)
        return carry

    lax.fori_loop(1, total, greet, 0)
    k_copy = pltpu.make_async_copy(k_ref, kt, local_sem.at[0])
    v_copy = pltpu.make_async_copy(v_ref, vt, local_sem.at[1])
    q_copy = pltpu.make_async_copy(q_ref.at[pl.ds(b * group, group)], qx.at[0], local_sem.at[2])
    w_copy = pltpu.make_async_copy(w_ref, wv, local_sem.at[3])
    k_copy.start()
    v_copy.start()
    q_copy.start()
    w_copy.start()
    pl.semaphore_wait(barrier, total - 1)

    y_me, x_me = b // nx, lax.rem(b, nx)

    def ahead(k):
        return lax.rem(y_me + k // nx, ny) * nx + lax.rem(x_me + k % nx, nx)

    def back(k):
        return (ny - k // nx) % ny * nx + (nx - k % nx) % nx

    def q_move(k):
        to = ahead(k)
        return pltpu.make_async_remote_copy(
            src_ref=q_ref.at[pl.ds(to * group, group)], dst_ref=qx.at[back(k)],
            send_sem=q_send.at[k], recv_sem=q_recv.at[back(k)],
            device_id=(to, c), device_id_type=MESH,
        )

    for k in range(1, nb):
        q_move(k).start()

    lane = lax.broadcasted_iota(jnp.int32, (size, LANES), 1) < size
    lane_x = lax.broadcasted_iota(jnp.int32, (EXTRA, LANES), 1) < size
    row_x = lax.broadcasted_iota(jnp.int32, (EXTRA, LANES), 0)
    ones = jnp.ones((EXTRA, tokens), jnp.bfloat16)

    def rs_move(k):
        to = lax.rem(c + k, nc)
        return pltpu.make_async_remote_copy(
            src_ref=part.at[to], dst_ref=rs.at[k],
            send_sem=rs_send.at[k], recv_sem=rs_recv.at[k],
            device_id=(b, to), device_id_type=MESH,
        )

    k_copy.wait()
    v_copy.wait()

    def partials(k, carry):
        to = lax.rem(c + k, nc)
        for i in range(ppd):
            at = pl.multiple_of((i * nc + to) * LANES, LANES)
            feature = softplus(kt[pl.ds(at, LANES), :])
            left = jnp.concatenate([vt[pl.ds(at, LANES), :], ones], axis=0)
            s = lax.dot_general(left, feature, (((1,), (1,)), ((), ())), preferred_element_type=jnp.float32)
            part[to, i, :size, :] = jnp.where(lane, s[:size], s[size : 2 * size]).astype(jnp.bfloat16)
            part[to, i, size:, :] = split_mass(s[2 * size :])

        @pl.when(k > 1)
        def _():
            rs_move(k - 1).start()

        return carry

    lax.fori_loop(1, nc + 1, partials, 0)

    for k in range(1, nc):
        rs_move(k).wait_recv()
    for i in range(ppd):
        s = part[c, i].astype(jnp.float32)
        for k in range(1, nc):
            s = s + rs[k, i].astype(jnp.float32)
        s = s / count
        own[i, :size, :] = s[:size].astype(jnp.bfloat16)
        m = jnp.broadcast_to(s[size : size + 1] + s[size + 1 : size + 2], (EXTRA, LANES))
        own[i, size:, :] = split_mass(m)

    def ag_move(i, k):
        p = i * nc + c
        g, slot = p // ppg, lax.rem(p, ppg)
        to = lax.rem(c + k, nc)
        landing = b * ppg + slot
        remote = pltpu.make_async_remote_copy(
            src_ref=own.at[i], dst_ref=st.at[landing],
            send_sem=ag_send.at[i * nc + k], recv_sem=ag_recv.at[landing],
            device_id=(g, to), device_id_type=MESH,
        )
        local = pltpu.make_async_copy(own.at[i], st.at[landing], ag_recv.at[landing])
        return g, remote, local

    for k in range(nc):
        for i in range(ppd):
            g, remote, local = ag_move(i, k)
            if k > 0:
                remote.start()
            else:
                pl.when(g != b)(remote.start)
                pl.when(g == b)(local.start)

    for k in range(nb):
        if k == 0:
            q_copy.wait()
        else:
            q_move(back(k)).wait_recv()

        def featured(i, carry):
            at = pl.multiple_of(i * LANES, LANES)
            qx[k, pl.ds(at, LANES), :] = softplus(qx[k, pl.ds(at, LANES), :])
            return carry

        lax.fori_loop(0, ppg, featured, 0)

    for k in range(nb):
        s = ahead(k)
        for slot in range(ppg):
            at = s * ppg + slot
            pltpu.make_async_copy(st.at[at], st.at[at], ag_recv.at[at]).wait()
            state = st[at, :size, :]
            mass = st[at, size:, :].astype(jnp.float32)
            hi, lo = mass[0:1], mass[1:2]
            low_half = jnp.where(lane_x, jnp.where(row_x == 0, hi, lo), 0.0)
            high_half = jnp.where(lane_x, 0.0, jnp.where(row_x == 2, hi, lo))
            m = jnp.where(row_x < 2, low_half, jnp.where(row_x < 4, high_half, 0.0)).astype(jnp.bfloat16)
            zero = jnp.zeros_like(state)
            left = jnp.concatenate([jnp.where(lane, state, zero), jnp.where(lane, zero, state), m], axis=0)
            both = lax.dot_general(
                left, qx[k, slot * LANES : (slot + 1) * LANES, :], (((1,), (0,)), ((), ())),
                preferred_element_type=jnp.float32,
            )
            low = both[2 * size :]
            first = count**0.5 / (low[0:1] + low[1:2] + 0.001)
            second = count**0.5 / (low[2:3] + low[3:4] + 0.001)
            read = jnp.concatenate([both[:size] * first, both[size : 2 * size] * second], axis=0)
            mixed[k * tokens : (k + 1) * tokens, slot * LANES : (slot + 1) * LANES] = read.T.astype(jnp.bfloat16)

    w_copy.wait()

    width = o_ref.shape[1] // chunks
    half = width // 2

    def place(axis, k):
        if axis == 0:
            return (y_me * nx + lax.rem(x_me + k, nx), c)
        return (lax.rem(y_me + k, ny) * nx + x_me, c)

    def offset(axis, k, other):
        return (other * nx + k) if axis == 0 else (k * nx + other)

    def first_move(j, h, k):
        n2 = ny if h == 0 else nx
        at = pl.ds((k - 1) * n2, n2)
        out_buf, in_buf, send, recv = stage1[h]
        return pltpu.make_async_remote_copy(
            src_ref=out_buf.at[j, at], dst_ref=in_buf.at[j, at],
            send_sem=send.at[j, k - 1], recv_sem=recv.at[j, k - 1],
            device_id=place(h, k), device_id_type=MESH,
        )

    def second_move(j, h, k):
        out_buf, in_buf, send, recv = stage2[h]
        return pltpu.make_async_remote_copy(
            src_ref=out_buf.at[j, k - 1], dst_ref=in_buf.at[j, k - 1],
            send_sem=send.at[j, k - 1], recv_sem=recv.at[j, k - 1],
            device_id=place(1 - h, k), device_id_type=MESH,
        )

    sizes = ((nx, ny), (ny, nx))

    def project(j, carry):
        at = pl.multiple_of(j * width, width)
        y = jnp.dot(mixed[...], wv[:, pl.ds(at, width)], preferred_element_type=jnp.float32)
        for h, (n1, n2) in enumerate(sizes):
            for k in range(n1):
                for other in range(n2):
                    r = offset(h, k, other) * tokens
                    piece = y[r : r + tokens, h * half : (h + 1) * half]
                    if k > 0:
                        stage1[h][0][j, (k - 1) * n2 + other] = piece.astype(jnp.bfloat16)
                    else:
                        mine[h][j, other] = piece
        for h, (n1, n2) in enumerate(sizes):
            for k in range(1, n1):
                first_move(j, h, k).start()
        return carry

    lax.fori_loop(0, chunks, project, 0)

    def relay(j, carry):
        for h, (n1, n2) in enumerate(sizes):
            for k in range(1, n1):
                first_move(j, h, k).wait_recv()
            for other in range(n2):
                y = mine[h][j, other]
                for k in range(1, n1):
                    y = y + stage1[h][1][j, (k - 1) * n2 + other].astype(jnp.float32)
                if other > 0:
                    stage2[h][0][j, other - 1] = y.astype(jnp.bfloat16)
                else:
                    mine[h][j, 0] = y
        for h, (n1, n2) in enumerate(sizes):
            for k in range(1, n2):
                second_move(j, h, k).start()
        return carry

    lax.fori_loop(0, chunks, relay, 0)

    def collect(j, carry):
        for h, (n1, n2) in enumerate(sizes):
            at = pl.multiple_of(j * width + h * half, half)
            y = mine[h][j, 0]
            for k in range(1, n2):
                second_move(j, h, k).wait_recv()
                y = y + stage2[h][1][j, k - 1].astype(jnp.float32)
            o_ref[:, pl.ds(at, half)] = y.astype(jnp.bfloat16)
        return carry

    lax.fori_loop(0, chunks, collect, 0)

    for k in range(1, nb):
        q_move(k).wait_send()

    def rs_end(k, carry):
        rs_move(k).wait_send()
        return carry

    lax.fori_loop(1, nc, rs_end, 0)
    for k in range(nc):
        for i in range(ppd):
            g, remote, local = ag_move(i, k)
            if k > 0:
                remote.wait_send()
            else:
                pl.when(g != b)(remote.wait_send)

    def pr_end(j, carry):
        for h, (n1, n2) in enumerate(sizes):
            for k in range(1, n1):
                first_move(j, h, k).wait_send()
            for k in range(1, n2):
                second_move(j, h, k).wait_send()
        return carry

    lax.fori_loop(0, chunks, pr_end, 0)


def solution(mesh):
    nb, nc = mesh.shape["batch"], mesh.shape["ctx"]
    nx = next(n for n in range(math.isqrt(nb), 0, -1) if nb % n == 0)
    ny = nb // nx

    def shards(asked_for, offered, contents, out_weight):
        _, tokens, heads, size = asked_for.shape
        rows = heads * size
        depth, columns = out_weight.shape
        pairs = rows // LANES
        block = size + EXTRA
        width = CHUNK if columns % CHUNK == 0 else columns
        chunks = columns // width

        def flat(x):
            return x.transpose(0, 2, 3, 1).reshape(rows, tokens)

        bf16, f32 = jnp.bfloat16, jnp.float32
        dma = pltpu.SemaphoreType.DMA
        sizes = ((nx, ny), (ny, nx))

        def stage(blocks, moves):
            buffer = pltpu.VMEM((chunks, blocks, tokens, width // 2), bf16)
            return [buffer, buffer, dma((chunks, moves)), dma((chunks, moves))]

        out = pl.pallas_call(
            functools.partial(kernel, ny, nx, nc, size),
            out_shape=jax.ShapeDtypeStruct((tokens, columns), bf16),
            in_specs=[pl.BlockSpec(memory_space=pl.ANY)] * 4,
            out_specs=pl.BlockSpec(memory_space=pltpu.VMEM),
            scratch_shapes=[
                pltpu.VMEM((rows, tokens), bf16),
                pltpu.VMEM((rows, tokens), bf16),
                pltpu.VMEM((depth, columns), bf16),
                pltpu.VMEM((nb, rows // nb, tokens), bf16),
                pltpu.VMEM((nc, pairs // nc, block, LANES), bf16),
                pltpu.VMEM((nc, pairs // nc, block, LANES), bf16),
                pltpu.VMEM((pairs // nc, block, LANES), bf16),
                pltpu.VMEM((pairs, block, LANES), bf16),
                pltpu.VMEM((nb * tokens, rows // nb), bf16),
                [pltpu.VMEM((chunks, n2, tokens, width // 2), f32) for _, n2 in sizes],
                [stage((n1 - 1) * n2, n1 - 1) for n1, n2 in sizes],
                [stage(n2 - 1, n2 - 1) for _, n2 in sizes],
                dma((4,)),
                dma((nb,)),
                dma((nb,)),
                dma((nc,)),
                dma((nc,)),
                dma((pairs,)),
                dma((pairs,)),
            ],
            compiler_params=pltpu.CompilerParams(
                collective_id=0, has_side_effects=True, vmem_limit_bytes=60 * 2**20
            ),
        )(flat(asked_for), flat(offered), flat(contents), out_weight)
        return out[None]

    in_specs = (
        P("batch", "ctx", None, None),
        P("batch", "ctx", None, None),
        P("batch", "ctx", None, None),
        P("batch", None),
    )
    return jax.shard_map(
        shards, mesh=mesh, in_specs=in_specs, out_specs=P("batch", "ctx", None), check_vma=False
    )
```

```python
import functools
import math

import jax
import jax.numpy as jnp
from jax import lax
from jax.experimental import pallas as pl
from jax.experimental.pallas import tpu as pltpu
from jax.sharding import PartitionSpec as P

MESH = pl.DeviceIdType.MESH
LANES = 128
EXTRA = 16
CHUNK = 512


def softplus(x):
    x = x.astype(jnp.float32)
    return (jnp.maximum(x, 0.0) + jnp.log(1.0 + jnp.exp(-jnp.abs(x)))).astype(jnp.bfloat16)


def split_mass(m):
    row = lax.broadcasted_iota(jnp.int32, (EXTRA, LANES), 0)
    high = m.astype(jnp.bfloat16).astype(jnp.float32)
    return jnp.where(row == 0, high, jnp.where(row == 1, m - high, 0.0)).astype(jnp.bfloat16)


def kernel(
    ny, nx, nc, size, q_ref, k_ref, v_ref, w_ref, o_ref,
    kt, vt, wv, qx, part, part_in, both, rs, own, st, mixed, mine, stage1, stage2,
    local_sem, q_send, q_recv, pa_send, pa_recv, rs_send, rs_recv,
    ag_send, ag_recv, fw_send, fw_recv,
):
    b, c = lax.axis_index("batch"), lax.axis_index("ctx")
    nb = ny * nx
    rows, tokens = k_ref.shape
    pairs = rows // LANES
    ppg, ppd = pairs // nb, pairs // nc
    group = rows // nb
    total = nb * nc
    me = b * nc + c
    count = tokens * nc
    chunks = mine[0].shape[0]

    barrier = pltpu.get_barrier_semaphore()

    def greet(i, carry):
        d = lax.rem(me + i, total)
        pl.semaphore_signal(barrier, inc=1, device_id=(d // nc, lax.rem(d, nc)), device_id_type=MESH)
        return carry

    lax.fori_loop(1, total, greet, 0)
    k_copy = pltpu.make_async_copy(k_ref, kt, local_sem.at[0])
    v_copy = pltpu.make_async_copy(v_ref, vt, local_sem.at[1])
    q_copy = pltpu.make_async_copy(q_ref.at[pl.ds(b * group, group)], qx.at[0], local_sem.at[2])
    w_copy = pltpu.make_async_copy(w_ref, wv, local_sem.at[3])
    k_copy.start()
    v_copy.start()
    q_copy.start()
    w_copy.start()
    pl.semaphore_wait(barrier, total - 1)

    y_me, x_me = b // nx, lax.rem(b, nx)

    def ahead(k):
        return lax.rem(y_me + k // nx, ny) * nx + lax.rem(x_me + k % nx, nx)

    def back(k):
        return (ny - k // nx) % ny * nx + (nx - k % nx) % nx

    def q_move(k):
        to = ahead(k)
        return pltpu.make_async_remote_copy(
            src_ref=q_ref.at[pl.ds(to * group, group)], dst_ref=qx.at[back(k)],
            send_sem=q_send.at[k], recv_sem=q_recv.at[back(k)],
            device_id=(to, c), device_id_type=MESH,
        )

    for k in range(1, nb):
        q_move(k).start()

    lane = lax.broadcasted_iota(jnp.int32, (size, LANES), 1) < size
    lane_x = lax.broadcasted_iota(jnp.int32, (EXTRA, LANES), 1) < size
    row_x = lax.broadcasted_iota(jnp.int32, (EXTRA, LANES), 0)
    ones = jnp.ones((EXTRA, tokens), jnp.bfloat16)

    nz, z_me, odd = nc // 2, c // 2, lax.rem(c, 2)
    partner = z_me * 2 + 1 - odd

    def pa_move(k):
        return pltpu.make_async_remote_copy(
            src_ref=part.at[k - 1], dst_ref=part_in.at[k - 1],
            send_sem=pa_send.at[k - 1], recv_sem=pa_recv.at[k - 1],
            device_id=(b, partner), device_id_type=MESH,
        )

    def rs_move(k):
        return pltpu.make_async_remote_copy(
            src_ref=both.at[k - 1], dst_ref=rs.at[k - 1],
            send_sem=rs_send.at[k - 1], recv_sem=rs_recv.at[k - 1],
            device_id=(b, lax.rem(z_me + k, nz) * 2 + odd), device_id_type=MESH,
        )

    def partial_sum(i, to):
        at = pl.multiple_of((i * nc + to) * LANES, LANES)
        feature = softplus(kt[pl.ds(at, LANES), :])
        left = jnp.concatenate([vt[pl.ds(at, LANES), :], ones], axis=0)
        s = lax.dot_general(left, feature, (((1,), (1,)), ((), ())), preferred_element_type=jnp.float32)
        return jnp.where(lane, s[:size], s[size : 2 * size]), s[2 * size :]

    def mass_of(block):
        return block[size : size + 1].astype(jnp.float32) + block[size + 1 : size + 2].astype(jnp.float32)

    k_copy.wait()
    v_copy.wait()

    def for_partner(k, carry):
        to = lax.rem(z_me + k, nz) * 2 + 1 - odd
        for i in range(ppd):
            state, mass = partial_sum(i, to)
            part[k - 1, i, :size, :] = state.astype(jnp.bfloat16)
            part[k - 1, i, size:, :] = split_mass(mass)

        @pl.when(k > 1)
        def _():
            pa_move(k - 1).start()

        return carry

    lax.fori_loop(1, nz + 1, for_partner, 0)
    pa_move(nz).start()

    def for_chip(k, carry):
        to = lax.rem(z_me + k, nz) * 2 + odd
        sums = [partial_sum(i, to) for i in range(ppd)]
        pa_move(k).wait_recv()
        for i, (state, mass) in enumerate(sums):
            block = part_in[k - 1, i]
            both[k - 1, i, :size, :] = (state + block[:size].astype(jnp.float32)).astype(jnp.bfloat16)
            both[k - 1, i, size:, :] = split_mass(mass + mass_of(block))

        @pl.when(k > 1)
        def _():
            rs_move(k - 1).start()

        return carry

    lax.fori_loop(1, nz + 1, for_chip, 0)

    for k in range(1, nz):
        rs_move(k).wait_recv()
    for i in range(ppd):
        blocks = [both[nz - 1, i]] + [rs[k - 1, i] for k in range(1, nz)]
        state = sum(x[:size].astype(jnp.float32) for x in blocks) / count
        mass = sum(mass_of(x) for x in blocks) / count
        own[i, :size, :] = state.astype(jnp.bfloat16)
        own[i, size:, :] = split_mass(jnp.broadcast_to(mass, (EXTRA, LANES)))

    def ag_move(i, k):
        p = i * nc + c
        g, slot = p // ppg, lax.rem(p, ppg)
        to = lax.rem(z_me + k, nz) * 2 + odd
        landing = b * ppg + slot
        remote = pltpu.make_async_remote_copy(
            src_ref=own.at[i], dst_ref=st.at[landing],
            send_sem=ag_send.at[i * nz + k], recv_sem=ag_recv.at[landing],
            device_id=(g, to), device_id_type=MESH,
        )
        local = pltpu.make_async_copy(own.at[i], st.at[landing], ag_recv.at[landing])
        return g, remote, local

    def fw_move(k, u):
        landing = ahead(k) * ppg + 2 * u + odd
        return pltpu.make_async_remote_copy(
            src_ref=st.at[landing], dst_ref=st.at[landing],
            send_sem=fw_send.at[landing], recv_sem=fw_recv.at[landing],
            device_id=(b, partner), device_id_type=MESH,
        )

    for k in range(nz):
        for i in range(ppd):
            g, remote, local = ag_move(i, k)
            if k > 0:
                remote.start()
            else:
                pl.when(g != b)(remote.start)
                pl.when(g == b)(local.start)

    for k in range(nb):
        if k == 0:
            q_copy.wait()
        else:
            q_move(back(k)).wait_recv()

        def featured(i, carry):
            at = pl.multiple_of(i * LANES, LANES)
            qx[k, pl.ds(at, LANES), :] = softplus(qx[k, pl.ds(at, LANES), :])
            return carry

        lax.fori_loop(0, ppg, featured, 0)

    def read(k, slot):
        at = ahead(k) * ppg + slot
        state = st[at, :size, :]
        mass = st[at, size:, :].astype(jnp.float32)
        hi, lo = mass[0:1], mass[1:2]
        low_half = jnp.where(lane_x, jnp.where(row_x == 0, hi, lo), 0.0)
        high_half = jnp.where(lane_x, 0.0, jnp.where(row_x == 2, hi, lo))
        m = jnp.where(row_x < 2, low_half, jnp.where(row_x < 4, high_half, 0.0)).astype(jnp.bfloat16)
        zero = jnp.zeros_like(state)
        left = jnp.concatenate([jnp.where(lane, state, zero), jnp.where(lane, zero, state), m], axis=0)
        column = pl.multiple_of(slot * LANES, LANES)
        y = lax.dot_general(
            left, qx[k, pl.ds(column, LANES), :], (((1,), (0,)), ((), ())),
            preferred_element_type=jnp.float32,
        )
        low = y[2 * size :]
        first = count**0.5 / (low[0:1] + low[1:2] + 0.001)
        second = count**0.5 / (low[2:3] + low[3:4] + 0.001)
        y = jnp.concatenate([y[:size] * first, y[size : 2 * size] * second], axis=0)
        mixed[k * tokens : (k + 1) * tokens, pl.ds(column, LANES)] = y.T.astype(jnp.bfloat16)

    for k in range(nb):
        for u in range(ppg // 2):
            at = ahead(k) * ppg + 2 * u + odd
            pltpu.make_async_copy(st.at[at], st.at[at], ag_recv.at[at]).wait()
            fw_move(k, u).start()
            read(k, 2 * u + odd)
    for k in range(nb):
        for u in range(ppg // 2):
            at = ahead(k) * ppg + 2 * u + 1 - odd
            pltpu.make_async_copy(st.at[at], st.at[at], fw_recv.at[at]).wait()
            read(k, 2 * u + 1 - odd)

    w_copy.wait()

    width = o_ref.shape[1] // chunks
    half = width // 2

    def place(axis, k):
        if axis == 0:
            return (y_me * nx + lax.rem(x_me + k, nx), c)
        return (lax.rem(y_me + k, ny) * nx + x_me, c)

    def offset(axis, k, other):
        return (other * nx + k) if axis == 0 else (k * nx + other)

    def first_move(j, h, k):
        n2 = ny if h == 0 else nx
        at = pl.ds((k - 1) * n2, n2)
        out_buf, in_buf, send, recv = stage1[h]
        return pltpu.make_async_remote_copy(
            src_ref=out_buf.at[j, at], dst_ref=in_buf.at[j, at],
            send_sem=send.at[j, k - 1], recv_sem=recv.at[j, k - 1],
            device_id=place(h, k), device_id_type=MESH,
        )

    def second_move(j, h, k):
        out_buf, in_buf, send, recv = stage2[h]
        return pltpu.make_async_remote_copy(
            src_ref=out_buf.at[j, k - 1], dst_ref=in_buf.at[j, k - 1],
            send_sem=send.at[j, k - 1], recv_sem=recv.at[j, k - 1],
            device_id=place(1 - h, k), device_id_type=MESH,
        )

    sizes = ((nx, ny), (ny, nx))

    def project(j, carry):
        at = pl.multiple_of(j * width, width)
        y = jnp.dot(mixed[...], wv[:, pl.ds(at, width)], preferred_element_type=jnp.float32)
        for h, (n1, n2) in enumerate(sizes):
            for k in range(n1):
                for other in range(n2):
                    r = offset(h, k, other) * tokens
                    piece = y[r : r + tokens, h * half : (h + 1) * half]
                    if k > 0:
                        stage1[h][0][j, (k - 1) * n2 + other] = piece.astype(jnp.bfloat16)
                    else:
                        mine[h][j, other] = piece
        for h, (n1, n2) in enumerate(sizes):
            for k in range(1, n1):
                first_move(j, h, k).start()
        return carry

    lax.fori_loop(0, chunks, project, 0)

    def relay(j, carry):
        for h, (n1, n2) in enumerate(sizes):
            for k in range(1, n1):
                first_move(j, h, k).wait_recv()
            for other in range(n2):
                y = mine[h][j, other]
                for k in range(1, n1):
                    y = y + stage1[h][1][j, (k - 1) * n2 + other].astype(jnp.float32)
                if other > 0:
                    stage2[h][0][j, other - 1] = y.astype(jnp.bfloat16)
                else:
                    mine[h][j, 0] = y
        for h, (n1, n2) in enumerate(sizes):
            for k in range(1, n2):
                second_move(j, h, k).start()
        return carry

    lax.fori_loop(0, chunks, relay, 0)

    def collect(j, carry):
        for h, (n1, n2) in enumerate(sizes):
            at = pl.multiple_of(j * width + h * half, half)
            y = mine[h][j, 0]
            for k in range(1, n2):
                second_move(j, h, k).wait_recv()
                y = y + stage2[h][1][j, k - 1].astype(jnp.float32)
            o_ref[:, pl.ds(at, half)] = y.astype(jnp.bfloat16)
        return carry

    lax.fori_loop(0, chunks, collect, 0)

    for k in range(1, nb):
        q_move(k).wait_send()

    for k in range(1, nz + 1):
        pa_move(k).wait_send()
    for k in range(1, nz):
        rs_move(k).wait_send()
    for k in range(nz):
        for i in range(ppd):
            g, remote, local = ag_move(i, k)
            if k > 0:
                remote.wait_send()
            else:
                pl.when(g != b)(remote.wait_send)
    for k in range(nb):
        for u in range(ppg // 2):
            fw_move(k, u).wait_send()

    def pr_end(j, carry):
        for h, (n1, n2) in enumerate(sizes):
            for k in range(1, n1):
                first_move(j, h, k).wait_send()
            for k in range(1, n2):
                second_move(j, h, k).wait_send()
        return carry

    lax.fori_loop(0, chunks, pr_end, 0)


def solution(mesh):
    nb, nc = mesh.shape["batch"], mesh.shape["ctx"]
    nx = next(n for n in range(math.isqrt(nb), 0, -1) if nb % n == 0)
    ny = nb // nx

    def shards(asked_for, offered, contents, out_weight):
        _, tokens, heads, size = asked_for.shape
        rows = heads * size
        depth, columns = out_weight.shape
        pairs = rows // LANES
        block = size + EXTRA
        width = CHUNK if columns % CHUNK == 0 else columns
        chunks = columns // width

        def flat(x):
            return x.transpose(0, 2, 3, 1).reshape(rows, tokens)

        bf16, f32 = jnp.bfloat16, jnp.float32
        dma = pltpu.SemaphoreType.DMA
        sizes = ((nx, ny), (ny, nx))

        def stage(blocks, moves):
            buffer = pltpu.VMEM((chunks, blocks, tokens, width // 2), bf16)
            return [buffer, buffer, dma((chunks, moves)), dma((chunks, moves))]

        out = pl.pallas_call(
            functools.partial(kernel, ny, nx, nc, size),
            out_shape=jax.ShapeDtypeStruct((tokens, columns), bf16),
            in_specs=[pl.BlockSpec(memory_space=pl.ANY)] * 4,
            out_specs=pl.BlockSpec(memory_space=pltpu.VMEM),
            scratch_shapes=[
                pltpu.VMEM((rows, tokens), bf16),
                pltpu.VMEM((rows, tokens), bf16),
                pltpu.VMEM((depth, columns), bf16),
                pltpu.VMEM((nb, rows // nb, tokens), bf16),
                pltpu.VMEM((nc // 2, pairs // nc, block, LANES), bf16),
                pltpu.VMEM((nc // 2, pairs // nc, block, LANES), bf16),
                pltpu.VMEM((nc // 2, pairs // nc, block, LANES), bf16),
                pltpu.VMEM((nc // 2, pairs // nc, block, LANES), bf16),
                pltpu.VMEM((pairs // nc, block, LANES), bf16),
                pltpu.VMEM((pairs, block, LANES), bf16),
                pltpu.VMEM((nb * tokens, rows // nb), bf16),
                [pltpu.VMEM((chunks, n2, tokens, width // 2), f32) for _, n2 in sizes],
                [stage((n1 - 1) * n2, n1 - 1) for n1, n2 in sizes],
                [stage(n2 - 1, n2 - 1) for _, n2 in sizes],
                dma((4,)),
                dma((nb,)),
                dma((nb,)),
                dma((nc // 2,)),
                dma((nc // 2,)),
                dma((nc // 2,)),
                dma((nc // 2,)),
                dma((pairs // 2,)),
                dma((pairs,)),
                dma((pairs,)),
                dma((pairs,)),
            ],
            compiler_params=pltpu.CompilerParams(
                collective_id=0, has_side_effects=True, vmem_limit_bytes=60 * 2**20
            ),
        )(flat(asked_for), flat(offered), flat(contents), out_weight)
        return out[None]

    in_specs = (
        P("batch", "ctx", None, None),
        P("batch", "ctx", None, None),
        P("batch", "ctx", None, None),
        P("batch", None),
    )
    return jax.shard_map(
        shards, mesh=mesh, in_specs=in_specs, out_specs=P("batch", "ctx", None), check_vma=False
    )
```

```python
import functools
import math

import jax
import jax.numpy as jnp
from jax import lax
from jax.experimental import pallas as pl
from jax.experimental.pallas import tpu as pltpu
from jax.sharding import PartitionSpec as P

MESH = pl.DeviceIdType.MESH
LANES = 128
EXTRA = 16
CHUNK = 256


def softplus(x):
    x = x.astype(jnp.float32)
    return (jnp.maximum(x, 0.0) + jnp.log(1.0 + jnp.exp(-jnp.abs(x)))).astype(jnp.bfloat16)


def split_mass(m):
    row = lax.broadcasted_iota(jnp.int32, (EXTRA, LANES), 0)
    high = m.astype(jnp.bfloat16).astype(jnp.float32)
    return jnp.where(row == 0, high, jnp.where(row == 1, m - high, 0.0)).astype(jnp.bfloat16)


def kernel(
    ny, nx, nc, size, q_ref, k_ref, v_ref, w_ref, o_ref,
    kt, vt, wv, qx, part, part_in, both, rs, own, st, mixed, mine, stage1, stage2,
    local_sem, q_send, q_recv, pa_send, pa_recv, rs_send, rs_recv,
    ag_send, ag_recv, fw_send, fw_recv,
):
    b, c = lax.axis_index("batch"), lax.axis_index("ctx")
    nb = ny * nx
    rows, tokens = k_ref.shape
    pairs = rows // LANES
    ppg, ppd = pairs // nb, pairs // nc
    group = rows // nb
    total = nb * nc
    me = b * nc + c
    count = tokens * nc
    chunks = mine[0].shape[0]

    barrier = pltpu.get_barrier_semaphore()

    def greet(i, carry):
        d = lax.rem(me + i, total)
        pl.semaphore_signal(barrier, inc=1, device_id=(d // nc, lax.rem(d, nc)), device_id_type=MESH)
        return carry

    lax.fori_loop(1, total, greet, 0)
    k_copy = pltpu.make_async_copy(k_ref, kt, local_sem.at[0])
    v_copy = pltpu.make_async_copy(v_ref, vt, local_sem.at[1])
    q_copy = pltpu.make_async_copy(q_ref.at[pl.ds(b * group, group)], qx.at[0], local_sem.at[2])
    w_copy = pltpu.make_async_copy(w_ref, wv, local_sem.at[3])
    k_copy.start()
    v_copy.start()
    q_copy.start()
    w_copy.start()
    pl.semaphore_wait(barrier, total - 1)

    y_me, x_me = b // nx, lax.rem(b, nx)

    def ahead(k):
        return lax.rem(y_me + k // nx, ny) * nx + lax.rem(x_me + k % nx, nx)

    def back(k):
        return (ny - k // nx) % ny * nx + (nx - k % nx) % nx

    def q_move(k):
        to = ahead(k)
        return pltpu.make_async_remote_copy(
            src_ref=q_ref.at[pl.ds(to * group, group)], dst_ref=qx.at[back(k)],
            send_sem=q_send.at[k], recv_sem=q_recv.at[back(k)],
            device_id=(to, c), device_id_type=MESH,
        )

    for k in range(1, nb):
        q_move(k).start()

    lane = lax.broadcasted_iota(jnp.int32, (size, LANES), 1) < size
    lane_x = lax.broadcasted_iota(jnp.int32, (EXTRA, LANES), 1) < size
    row_x = lax.broadcasted_iota(jnp.int32, (EXTRA, LANES), 0)
    ones = jnp.ones((EXTRA, tokens), jnp.bfloat16)

    nz, z_me, odd = nc // 2, c // 2, lax.rem(c, 2)
    partner = z_me * 2 + 1 - odd

    def pa_move(k):
        return pltpu.make_async_remote_copy(
            src_ref=part.at[k - 1], dst_ref=part_in.at[k - 1],
            send_sem=pa_send.at[k - 1], recv_sem=pa_recv.at[k - 1],
            device_id=(b, partner), device_id_type=MESH,
        )

    def rs_move(k):
        return pltpu.make_async_remote_copy(
            src_ref=both.at[k - 1], dst_ref=rs.at[k - 1],
            send_sem=rs_send.at[k - 1], recv_sem=rs_recv.at[k - 1],
            device_id=(b, lax.rem(z_me + k, nz) * 2 + odd), device_id_type=MESH,
        )

    def partial_sum(i, to):
        at = pl.multiple_of((i * nc + to) * LANES, LANES)
        feature = softplus(kt[pl.ds(at, LANES), :])
        left = jnp.concatenate([vt[pl.ds(at, LANES), :], ones], axis=0)
        s = lax.dot_general(left, feature, (((1,), (1,)), ((), ())), preferred_element_type=jnp.float32)
        return jnp.where(lane, s[:size], s[size : 2 * size]), s[2 * size :]

    def mass_of(block):
        return block[size : size + 1].astype(jnp.float32) + block[size + 1 : size + 2].astype(jnp.float32)

    k_copy.wait()
    v_copy.wait()

    for k in range(1, nz + 1):
        to = lax.rem(z_me + k, nz) * 2 + 1 - odd
        for i in range(ppd):
            state, mass = partial_sum(i, to)
            part[k - 1, i, :size, :] = state.astype(jnp.bfloat16)
            part[k - 1, i, size:, :] = split_mass(mass)
        if k > 1:
            pa_move(k - 1).start()
    pa_move(nz).start()

    for k in range(1, nz + 1):
        to = lax.rem(z_me + k, nz) * 2 + odd
        sums = [partial_sum(i, to) for i in range(ppd)]
        pa_move(k).wait_recv()
        for i, (state, mass) in enumerate(sums):
            block = part_in[k - 1, i]
            both[k - 1, i, :size, :] = (state + block[:size].astype(jnp.float32)).astype(jnp.bfloat16)
            both[k - 1, i, size:, :] = split_mass(mass + mass_of(block))
        if k > 1:
            rs_move(k - 1).start()

    for k in range(1, nz):
        rs_move(k).wait_recv()
    for i in range(ppd):
        blocks = [both[nz - 1, i]] + [rs[k - 1, i] for k in range(1, nz)]
        state = sum(x[:size].astype(jnp.float32) for x in blocks) / count
        mass = sum(mass_of(x) for x in blocks) / count
        own[i, :size, :] = state.astype(jnp.bfloat16)
        own[i, size:, :] = split_mass(jnp.broadcast_to(mass, (EXTRA, LANES)))

    def ag_move(i, k):
        p = i * nc + c
        g, slot = p // ppg, lax.rem(p, ppg)
        to = lax.rem(z_me + k, nz) * 2 + odd
        landing = b * ppg + slot
        remote = pltpu.make_async_remote_copy(
            src_ref=own.at[i], dst_ref=st.at[landing],
            send_sem=ag_send.at[i * nz + k], recv_sem=ag_recv.at[landing],
            device_id=(g, to), device_id_type=MESH,
        )
        local = pltpu.make_async_copy(own.at[i], st.at[landing], ag_recv.at[landing])
        return g, remote, local

    def fw_move(k, u):
        landing = ahead(k) * ppg + 2 * u + odd
        return pltpu.make_async_remote_copy(
            src_ref=st.at[landing], dst_ref=st.at[landing],
            send_sem=fw_send.at[landing], recv_sem=fw_recv.at[landing],
            device_id=(b, partner), device_id_type=MESH,
        )

    for k in range(nz):
        for i in range(ppd):
            g, remote, local = ag_move(i, k)
            if k > 0:
                remote.start()
            else:
                pl.when(g != b)(remote.start)
                pl.when(g == b)(local.start)

    for k in range(nb):
        if k == 0:
            q_copy.wait()
        else:
            q_move(back(k)).wait_recv()

        def featured(i, carry):
            at = pl.multiple_of(i * LANES, LANES)
            qx[k, pl.ds(at, LANES), :] = softplus(qx[k, pl.ds(at, LANES), :])
            return carry

        lax.fori_loop(0, ppg, featured, 0)

    def read(k, slot):
        at = ahead(k) * ppg + slot
        state = st[at, :size, :]
        mass = st[at, size:, :].astype(jnp.float32)
        hi, lo = mass[0:1], mass[1:2]
        low_half = jnp.where(lane_x, jnp.where(row_x == 0, hi, lo), 0.0)
        high_half = jnp.where(lane_x, 0.0, jnp.where(row_x == 2, hi, lo))
        m = jnp.where(row_x < 2, low_half, jnp.where(row_x < 4, high_half, 0.0)).astype(jnp.bfloat16)
        zero = jnp.zeros_like(state)
        left = jnp.concatenate([jnp.where(lane, state, zero), jnp.where(lane, zero, state), m], axis=0)
        column = pl.multiple_of(slot * LANES, LANES)
        y = lax.dot_general(
            left, qx[k, pl.ds(column, LANES), :], (((1,), (0,)), ((), ())),
            preferred_element_type=jnp.float32,
        )
        low = y[2 * size :]
        first = count**0.5 / (low[0:1] + low[1:2] + 0.001)
        second = count**0.5 / (low[2:3] + low[3:4] + 0.001)
        y = jnp.concatenate([y[:size] * first, y[size : 2 * size] * second], axis=0)
        mixed[k * tokens : (k + 1) * tokens, pl.ds(column, LANES)] = y.T.astype(jnp.bfloat16)

    for k in range(nb):
        for u in range(ppg // 2):
            at = ahead(k) * ppg + 2 * u + odd
            pltpu.make_async_copy(st.at[at], st.at[at], ag_recv.at[at]).wait()
            fw_move(k, u).start()
            read(k, 2 * u + odd)
    for k in range(nb):
        for u in range(ppg // 2):
            at = ahead(k) * ppg + 2 * u + 1 - odd
            pltpu.make_async_copy(st.at[at], st.at[at], fw_recv.at[at]).wait()
            read(k, 2 * u + 1 - odd)

    w_copy.wait()

    width = o_ref.shape[1] // chunks
    half = width // 2

    def place(axis, k):
        if axis == 0:
            return (y_me * nx + lax.rem(x_me + k, nx), c)
        return (lax.rem(y_me + k, ny) * nx + x_me, c)

    def offset(axis, k, other):
        return (other * nx + k) if axis == 0 else (k * nx + other)

    def first_move(j, h, k):
        n2 = ny if h == 0 else nx
        at = pl.ds((k - 1) * n2, n2)
        out_buf, in_buf, send, recv = stage1[h]
        return pltpu.make_async_remote_copy(
            src_ref=out_buf.at[j, at], dst_ref=in_buf.at[j, at],
            send_sem=send.at[j, k - 1], recv_sem=recv.at[j, k - 1],
            device_id=place(h, k), device_id_type=MESH,
        )

    def second_move(j, h, k):
        out_buf, in_buf, send, recv = stage2[h]
        return pltpu.make_async_remote_copy(
            src_ref=out_buf.at[j, k - 1], dst_ref=in_buf.at[j, k - 1],
            send_sem=send.at[j, k - 1], recv_sem=recv.at[j, k - 1],
            device_id=place(1 - h, k), device_id_type=MESH,
        )

    sizes = ((nx, ny), (ny, nx))

    def project(j, carry):
        at = pl.multiple_of(j * width, width)
        y = jnp.dot(mixed[...], wv[:, pl.ds(at, width)], preferred_element_type=jnp.float32)
        for h, (n1, n2) in enumerate(sizes):
            for k in range(n1):
                for other in range(n2):
                    r = offset(h, k, other) * tokens
                    piece = y[r : r + tokens, h * half : (h + 1) * half]
                    if k > 0:
                        stage1[h][0][j, (k - 1) * n2 + other] = piece.astype(jnp.bfloat16)
                    else:
                        mine[h][j, other] = piece
        for h, (n1, n2) in enumerate(sizes):
            for k in range(1, n1):
                first_move(j, h, k).start()
        return carry

    lax.fori_loop(0, chunks, project, 0)

    def relay(j, carry):
        for h, (n1, n2) in enumerate(sizes):
            for k in range(1, n1):
                first_move(j, h, k).wait_recv()
            for other in range(n2):
                y = mine[h][j, other]
                for k in range(1, n1):
                    y = y + stage1[h][1][j, (k - 1) * n2 + other].astype(jnp.float32)
                if other > 0:
                    stage2[h][0][j, other - 1] = y.astype(jnp.bfloat16)
                else:
                    mine[h][j, 0] = y
        for h, (n1, n2) in enumerate(sizes):
            for k in range(1, n2):
                second_move(j, h, k).start()
        return carry

    lax.fori_loop(0, chunks, relay, 0)

    def collect(j, carry):
        for h, (n1, n2) in enumerate(sizes):
            at = pl.multiple_of(j * width + h * half, half)
            y = mine[h][j, 0]
            for k in range(1, n2):
                second_move(j, h, k).wait_recv()
                y = y + stage2[h][1][j, k - 1].astype(jnp.float32)
            o_ref[:, pl.ds(at, half)] = y.astype(jnp.bfloat16)
        return carry

    lax.fori_loop(0, chunks, collect, 0)

    for k in range(1, nb):
        q_move(k).wait_send()

    for k in range(1, nz + 1):
        pa_move(k).wait_send()
    for k in range(1, nz):
        rs_move(k).wait_send()
    for k in range(nz):
        for i in range(ppd):
            g, remote, local = ag_move(i, k)
            if k > 0:
                remote.wait_send()
            else:
                pl.when(g != b)(remote.wait_send)
    for k in range(nb):
        for u in range(ppg // 2):
            fw_move(k, u).wait_send()

    def pr_end(j, carry):
        for h, (n1, n2) in enumerate(sizes):
            for k in range(1, n1):
                first_move(j, h, k).wait_send()
            for k in range(1, n2):
                second_move(j, h, k).wait_send()
        return carry

    lax.fori_loop(0, chunks, pr_end, 0)


def solution(mesh):
    nb, nc = mesh.shape["batch"], mesh.shape["ctx"]
    nx = next(n for n in range(math.isqrt(nb), 0, -1) if nb % n == 0)
    ny = nb // nx

    def shards(asked_for, offered, contents, out_weight):
        _, tokens, heads, size = asked_for.shape
        rows = heads * size
        depth, columns = out_weight.shape
        pairs = rows // LANES
        block = size + EXTRA
        width = CHUNK if columns % CHUNK == 0 else columns
        chunks = columns // width

        def flat(x):
            return x.transpose(0, 2, 3, 1).reshape(rows, tokens)

        bf16, f32 = jnp.bfloat16, jnp.float32
        dma = pltpu.SemaphoreType.DMA
        sizes = ((nx, ny), (ny, nx))

        def stage(blocks, moves):
            buffer = pltpu.VMEM((chunks, blocks, tokens, width // 2), bf16)
            return [buffer, buffer, dma((chunks, moves)), dma((chunks, moves))]

        out = pl.pallas_call(
            functools.partial(kernel, ny, nx, nc, size),
            out_shape=jax.ShapeDtypeStruct((tokens, columns), bf16),
            in_specs=[pl.BlockSpec(memory_space=pl.ANY)] * 4,
            out_specs=pl.BlockSpec(memory_space=pltpu.VMEM),
            scratch_shapes=[
                pltpu.VMEM((rows, tokens), bf16),
                pltpu.VMEM((rows, tokens), bf16),
                pltpu.VMEM((depth, columns), bf16),
                pltpu.VMEM((nb, rows // nb, tokens), bf16),
                pltpu.VMEM((nc // 2, pairs // nc, block, LANES), bf16),
                pltpu.VMEM((nc // 2, pairs // nc, block, LANES), bf16),
                pltpu.VMEM((nc // 2, pairs // nc, block, LANES), bf16),
                pltpu.VMEM((nc // 2, pairs // nc, block, LANES), bf16),
                pltpu.VMEM((pairs // nc, block, LANES), bf16),
                pltpu.VMEM((pairs, block, LANES), bf16),
                pltpu.VMEM((nb * tokens, rows // nb), bf16),
                [pltpu.VMEM((chunks, n2, tokens, width // 2), f32) for _, n2 in sizes],
                [stage((n1 - 1) * n2, n1 - 1) for n1, n2 in sizes],
                [stage(n2 - 1, n2 - 1) for _, n2 in sizes],
                dma((4,)),
                dma((nb,)),
                dma((nb,)),
                dma((nc // 2,)),
                dma((nc // 2,)),
                dma((nc // 2,)),
                dma((nc // 2,)),
                dma((pairs // 2,)),
                dma((pairs,)),
                dma((pairs,)),
                dma((pairs,)),
            ],
            compiler_params=pltpu.CompilerParams(
                collective_id=0, has_side_effects=True, vmem_limit_bytes=60 * 2**20
            ),
        )(flat(asked_for), flat(offered), flat(contents), out_weight)
        return out[None]

    in_specs = (
        P("batch", "ctx", None, None),
        P("batch", "ctx", None, None),
        P("batch", "ctx", None, None),
        P("batch", None),
    )
    return jax.shard_map(
        shards, mesh=mesh, in_specs=in_specs, out_specs=P("batch", "ctx", None), check_vma=False
    )
```
